32 devices in a mesh: groups: 2 (over y), ep: 16 (over z, x, core).
Axes of the slice: x: 2, y: 2, z: 4, core: 2. Of those that a mesh axis runs over, the one named last changes fastest.
Arguments:
- tokens: bfloat16 [128, 7168], P(('groups', 'ep')), parts along dimension 0, may hold values from -6 to 6
- routes: int32 [128, 8], P(('groups', 'ep')), parts along dimension 0, may hold values from 0 to 15, as said below
- gates: float32 [128, 8], P(('groups', 'ep')), parts along dimension 0, may hold values from 0.05 to 0.6
- gate_weight: bfloat16 [7168, 32768], P(None, 'ep'), may hold values from -0.0625 to 0.0625
- up_weight: bfloat16 [7168, 32768], P(None, 'ep'), may hold values from -0.0625 to 0.0625
- down_weight: bfloat16 [32768, 7168], P('ep'), may hold values from -0.125 to 0.125
Outputs:
- mixed: bfloat16 [128, 7168], P(('groups', 'ep')), parts along dimension 0
The draws below stay inside these ranges and needn't reach their ends.
There are 2 independent parts, one for each index of `groups`. The reference program is written for one: setup_inputs(seed, part) draws one part's arguments, and reference() takes and returns one part's arrays. A program takes and returns all parts, laid end to end along the dimension named above; an argument that names none is the same for every part. Nothing has to cross between parts.
Inputs may be any that keep to these rules, and one draw needn't show every extreme that they name: `routes`: each token names 8 different experts. Among the 4 tokens of one device no expert is named by more than 3 of them, and in every draw one expert is named by exactly 3 tokens of every device.
All inputs are finite; a program needn't handle non-finite values.
Results may differ from the reference program's by a relative error of at most 0.0085.
Values may be sent and summed in bfloat16 or wider, within the bound.
A program may use at most 128 MiB of HBM per device.

```python
import math
import jax
import jax.numpy as jnp
from jax import lax

D = 7168
FF = 2048
TOP = 8
EXPERTS = 16
TOK_DEV = 4
CAP = 3
TOKENS = 64


def draw_routes(key, part):
    hot_expert = jax.random.randint(jax.random.fold_in(key, 11), (), 0, EXPERTS).astype(jnp.int32)
    blocks = TOKENS // TOK_DEV
    block_keys = jax.random.split(jax.random.fold_in(key, 12), blocks)
    others = (hot_expert + 1 + jnp.arange(EXPERTS - 1, dtype=jnp.int32)) % EXPERTS
    expert_pool = jnp.repeat(others, CAP)

    def one_block(block_key):
        key_pool, key_rows, key_cols = jax.random.split(block_key, 3)
        shuffled = expert_pool[jax.random.permutation(key_pool, expert_pool.shape[0])]
        chosen = jnp.concatenate([jnp.full((CAP,), hot_expert, jnp.int32), shuffled[:TOK_DEV * TOP - CAP]])
        ordered = jnp.sort(chosen)
        route_table = ordered.reshape(TOP, TOK_DEV).T
        route_table = route_table[jax.random.permutation(key_rows, TOK_DEV)]
        scores = jax.random.randint(key_cols, (TOK_DEV, TOP), 0, 1 << 20) * TOP + jnp.arange(TOP, dtype=jnp.int32)[None, :]
        return jnp.take_along_axis(route_table, jnp.argsort(scores, axis=1), axis=1)
    return jax.vmap(one_block)(block_keys).reshape(TOKENS, TOP).astype(jnp.int32)


def level_of(rng, dims, cuts, low, top_value):
    level = 1.0
    for dim, blocks in cuts:
        draws = jax.random.uniform(jax.random.fold_in(jax.random.fold_in(rng, 6), dim), (blocks,), jnp.float32, low / len(cuts), top_value / len(cuts))
        level = level * jnp.repeat(jnp.exp(draws), dims[dim] // blocks).reshape((-1,) + (1,) * (len(dims) - 1 - dim))
    return level


def gaussian(key, dims, deviation, most, cuts=(), kind=jnp.bfloat16):
    gain = level_of(key, dims, cuts, -0.22, 0.18) if cuts else 1.0
    entries = jax.random.normal(key, dims, jnp.float32) * deviation * gain
    return jnp.minimum(jnp.maximum(entries, -most), most).astype(kind)


def setup_inputs(seed: int = 0, part: int = 0) -> dict:
    streams_of = jax.random.split(jax.random.key(seed), 7)
    part_splits = jax.random.split(jax.random.fold_in(streams_of[6], part), 7)
    return {
        "tokens": gaussian(part_splits[0], (TOKENS, D), 1.0, 6.0, ((0, 16),)),
        "routes": draw_routes(jax.random.fold_in(jax.random.fold_in(streams_of[6], part), 71), part),
        "gates": jnp.clip(jnp.exp(math.log(0.6) - 2.4849067 * jax.random.uniform(part_splits[2], (TOKENS, TOP), jnp.float32) ** level_of(part_splits[2], (TOKENS, TOP), ((0, 16),), -0.2, 0.2)), 0.05, 0.6),
        "gate_weight": gaussian(streams_of[3], (D, EXPERTS * FF), D ** -0.5, 0.0625, ((1, 16),)),
        "up_weight": gaussian(streams_of[4], (D, EXPERTS * FF), D ** -0.5, 0.0625, ((1, 16),)),
        "down_weight": gaussian(streams_of[5], (EXPERTS * FF, D), FF ** -0.5, 0.125, ((0, 16),)),
    }


def reference(tokens, routes, gates, gate_weight, up_weight, down_weight):
    bound = CAP * (TOKENS // TOK_DEV)

    def add_expert(running, expert):
        matches = routes == expert
        routed = jnp.any(matches, axis=1)
        weight = jnp.sum(jnp.where(matches, gates, jnp.zeros_like(gates)), axis=1)
        row_order = jnp.argsort(jnp.where(routed, 0, 1).astype(jnp.int32), stable=True)[:bound].astype(jnp.int32)
        picked_rows = tokens[row_order]
        start = (expert * FF).astype(jnp.int32)
        gate_cols = lax.dynamic_slice_in_dim(gate_weight, start, FF, 1)
        up_cols = lax.dynamic_slice_in_dim(up_weight, start, FF, 1)
        down_rows = lax.dynamic_slice_in_dim(down_weight, start, FF, 0)
        gate_act = jnp.dot(picked_rows, gate_cols, preferred_element_type=jnp.float32)
        up_act = jnp.dot(picked_rows, up_cols, preferred_element_type=jnp.float32)
        hidden = (jax.nn.silu(gate_act) * up_act).astype(jnp.bfloat16)
        expert_out = jnp.dot(hidden, down_rows, preferred_element_type=jnp.float32)
        running = running.at[row_order].add(weight[row_order][:, None] * expert_out)
        return running, None

    initial = jnp.zeros(tokens.shape, jnp.float32)
    running, unused = lax.scan(add_expert, initial, jnp.arange(EXPERTS, dtype=jnp.int32))
    return running.astype(jnp.bfloat16)
```

```python
import functools

import jax
import jax.numpy as jnp
from jax import lax
from jax.experimental import pallas as pl
from jax.experimental.pallas import tpu as pltpu
from jax.sharding import PartitionSpec as P

EXPERTS = 16
SLOTS = 3
AUX = 128


def piece(total, want):
    size = want
    while total % size:
        size //= 2
    return size


def kernel(
    devices, kc, nc, tile,
    tokens, routes, gates, wg, wu, wd, out,
    ring_g, ring_u, down, rx, ax, xf, xb, acc_g, acc_u, hid, share, mine, theirs, sbuf, rbuf,
    tok_sem, g_sem, u_sem, d_sem,
    tx_send, tx_recv, re_send, re_recv, ob_send, ob_recv, rt_send, rt_recv, ax_send, ax_recv,
):
    rows, width = tokens.shape
    hidden = wg.shape[1]
    chips = devices // 2
    units, outs = width // kc, width // nc
    me = lax.axis_index("ep")
    chip, core = me // 2, me % 2
    other = 1 - core
    peer = chip * 2 + other
    mates = chips * rows

    def remote(src, dst, send, recv, dev):
        return pltpu.make_async_remote_copy(
            src_ref=src, dst_ref=dst, send_sem=send, recv_sem=recv,
            device_id={"ep": dev}, device_id_type=pl.DeviceIdType.MESH,
        )

    def load_tokens(j):
        return pltpu.make_async_copy(
            tokens.at[:, pl.ds(j * kc, kc)], rx.at[j, core, chip], tok_sem.at[j]
        )

    def load_g(j):
        s = j % SLOTS
        return pltpu.make_async_copy(wg.at[pl.ds(j * kc, kc), :], ring_g.at[s], g_sem.at[s])

    def load_u(j):
        s = j % SLOTS
        return pltpu.make_async_copy(wu.at[pl.ds(j * kc, kc), :], ring_u.at[s], u_sem.at[s])

    def load_d(c):
        return pltpu.make_async_copy(wd.at[:, pl.ds(c * nc, nc)], down.at[c], d_sem.at[c])

    for j in range(units):
        load_tokens(j).start()
    for j in range(min(SLOTS, units)):
        load_g(j).start()
        load_u(j).start()

    barrier = pltpu.get_barrier_semaphore()
    pl.semaphore_signal(barrier, inc=1, device_id={"ep": peer}, device_id_type=pl.DeviceIdType.MESH)

    @pl.loop(1, chips)
    def _(i):
        to = lax.rem(chip + i, chips) * 2 + core
        pl.semaphore_signal(barrier, inc=1, device_id={"ep": to}, device_id_type=pl.DeviceIdType.MESH)

    lane = lax.broadcasted_iota(jnp.int32, (rows, AUX), 1)
    name = jnp.where(lane < EXPERTS, lane, lane - EXPERTS)
    weight = jnp.zeros((rows, AUX), jnp.float32)
    for k in range(routes.shape[1]):
        weight = weight + jnp.where(routes[:, k : k + 1] == name, gates[:, k : k + 1], 0.0)
    high = weight.astype(jnp.bfloat16).astype(jnp.float32)
    ax[core, chip] = jnp.where(
        lane < EXPERTS, high, jnp.where(lane < 2 * EXPERTS, weight - high, 0.0)
    ).astype(jnp.bfloat16)

    pl.semaphore_wait(barrier, chips)

    for j in range(units):
        load_tokens(j).wait()

        @pl.loop(1, chips)
        def _(i):
            to = lax.rem(chip + i, chips) * 2 + core
            remote(rx.at[j, core, chip], rx.at[j, core, chip], tx_send.at[j], tx_recv.at[j], to).start()

    @pl.loop(1, chips)
    def _(i):
        to = lax.rem(chip + i, chips) * 2 + core
        remote(ax.at[core, chip], ax.at[core, chip], ax_send.at[0], ax_recv.at[0], to).start()

    def many(ref, sem):
        return pltpu.make_async_copy(ref, ref, sem)

    def relay(j):
        return remote(rx.at[j, core], rx.at[j, core], re_send.at[j], re_recv.at[j], peer)

    relay_aux = remote(ax.at[core], ax.at[core], ax_send.at[1], ax_recv.at[1], peer)

    def forward(j):
        many(rx.at[j, 0, pl.ds(0, chips - 1)], tx_recv.at[j]).wait()
        relay(j).start()

    forward(0)
    for c in range(min(1, outs)):
        load_d(c).start()
    issued = 1
    for j in range(units):
        if j + 1 < units:
            forward(j + 1)
        else:
            many(ax.at[0, pl.ds(0, chips - 1)], ax_recv.at[0]).wait()
            relay_aux.start()
        relay(j).wait_recv()
        for half in range(2):
            @pl.loop(0, chips // 2)
            def _(b):
                pair = jnp.concatenate(
                    [rx[j, half, 2 * b].astype(jnp.float32), rx[j, half, 2 * b + 1].astype(jnp.float32)], axis=0
                )
                at = pl.multiple_of(half * mates + b * 2 * rows, 2 * rows)
                xf[pl.ds(at, 2 * rows), :] = pair
        xb[...] = xf[...].astype(jnp.bfloat16)
        load_g(j).wait()
        load_u(j).wait()
        s = j % SLOTS

        @pl.loop(0, hidden // tile)
        def _(n):
            cols = pl.ds(pl.multiple_of(n * tile, tile), tile)
            pg = jnp.dot(xb[...], ring_g[s, :, cols], preferred_element_type=jnp.float32)
            pu = jnp.dot(xb[...], ring_u[s, :, cols], preferred_element_type=jnp.float32)
            if j == 0:
                acc_g[:, cols] = pg
                acc_u[:, cols] = pu
            elif j < units - 1:
                acc_g[:, cols] += pg
                acc_u[:, cols] += pu
            else:
                g = acc_g[:, cols] + pg
                u = acc_u[:, cols] + pu
                hid[:, cols] = (g / (1.0 + jnp.exp(-g)) * u).astype(jnp.bfloat16)

        if j + SLOTS < units:
            load_g(j + SLOTS).start()
            load_u(j + SLOTS).start()
        goal = outs if j + SLOTS + 1 >= units else min(outs, issued + 1)
        while issued < goal:
            load_d(issued).start()
            issued += 1
    while issued < outs:
        load_d(issued).start()
        issued += 1

    relay_aux.wait_recv()
    expert = me // (devices // EXPERTS)
    spot = lax.broadcasted_iota(jnp.int32, (2 * rows, AUX), 1)
    hot = (spot == expert) | (spot == expert + EXPERTS)
    for half in range(2):
        @pl.loop(0, chips // 2)
        def _(b):
            pair = jnp.concatenate(
                [ax[half, 2 * b].astype(jnp.float32), ax[half, 2 * b + 1].astype(jnp.float32)], axis=0
            )
            at = pl.multiple_of(half * mates + b * 2 * rows, 2 * rows)
            total = jnp.sum(jnp.where(hot, pair, 0.0), axis=1, keepdims=True)
            share[pl.ds(at, 2 * rows), :] = jnp.broadcast_to(total, (2 * rows, AUX))

    def swap(c):
        return remote(mine.at[c, other], theirs.at[c], ob_send.at[c], ob_recv.at[c], peer)

    def give(c):
        swap(c).wait_recv()

        @pl.loop(0, chips // 2)
        def _(b):
            at = pl.multiple_of(b * 2 * rows, 2 * rows)
            both = mine[c, core, pl.ds(at, 2 * rows), :] + theirs[c, pl.ds(at, 2 * rows), :]
            sbuf[c, 2 * b] = both[:rows].astype(jnp.bfloat16)
            sbuf[c, 2 * b + 1] = both[rows:].astype(jnp.bfloat16)

        @pl.loop(1, chips)
        def _(i):
            dest = lax.rem(chip + i, chips)
            remote(
                sbuf.at[c, dest], rbuf.at[c, chip], rt_send.at[c], rt_recv.at[c], dest * 2 + core
            ).start()

        rbuf[c, chip] = sbuf[c, chip]

    sub = min(tile, nc)
    for c in range(outs):
        load_d(c).wait()

        @pl.loop(0, nc // sub)
        def _(n):
            cols = pl.ds(pl.multiple_of(n * sub, sub), sub)
            o = jnp.dot(hid[...], down[c, :, cols], preferred_element_type=jnp.float32)
            o = o * share[:, :1]
            mine[c, 0, :, cols] = o[:mates]
            mine[c, 1, :, cols] = o[mates:]

        swap(c).start()
        if c > 0:
            give(c - 1)
    give(outs - 1)

    for c in range(outs):
        many(rbuf.at[c, pl.ds(0, chips - 1)], rt_recv.at[c]).wait()
        total = rbuf[c, 0].astype(jnp.float32)
        if chips <= 16:
            for b in range(1, chips):
                total = total + rbuf[c, b].astype(jnp.float32)
        else:
            total = lax.fori_loop(1, chips, lambda b, t: t + rbuf[c, b].astype(jnp.float32), total)
        out[:, c * nc : (c + 1) * nc] = total.astype(jnp.bfloat16)

    for j in range(units):
        many(rx.at[j, 0, pl.ds(0, chips - 1)], tx_send.at[j]).wait()
        relay(j).wait_send()
    many(ax.at[0, pl.ds(0, chips - 1)], ax_send.at[0]).wait()
    relay_aux.wait_send()
    for c in range(outs):
        swap(c).wait_send()
        many(rbuf.at[c, pl.ds(0, chips - 1)], rt_send.at[c]).wait()


def layer(tokens, routes, gates, wg, wu, wd):
    devices = lax.axis_size("ep")
    rows, width = tokens.shape
    hidden = wg.shape[1]
    chips = devices // 2
    kc, nc = piece(width, 1024), piece(width, 1024)
    tile = piece(hidden, 512)
    units, outs = width // kc, width // nc
    batch = devices * rows
    bf16, f32 = jnp.bfloat16, jnp.float32
    dma = pltpu.SemaphoreType.DMA
    anywhere = pl.BlockSpec(memory_space=pl.ANY)
    vmem = pl.BlockSpec(memory_space=pltpu.VMEM)
    return pl.pallas_call(
        functools.partial(kernel, devices, kc, nc, tile),
        out_shape=jax.ShapeDtypeStruct((rows, width), bf16),
        in_specs=[anywhere, vmem, vmem, anywhere, anywhere, anywhere],
        out_specs=vmem,
        scratch_shapes=[
            pltpu.VMEM((SLOTS, kc, hidden), bf16),
            pltpu.VMEM((SLOTS, kc, hidden), bf16),
            pltpu.VMEM((outs, hidden, nc), bf16),
            pltpu.VMEM((units, 2, chips, rows, kc), bf16),
            pltpu.VMEM((2, chips, rows, AUX), bf16),
            pltpu.VMEM((batch, kc), f32),
            pltpu.VMEM((batch, kc), bf16),
            pltpu.VMEM((batch, hidden), f32),
            pltpu.VMEM((batch, hidden), f32),
            pltpu.VMEM((batch, hidden), bf16),
            pltpu.VMEM((batch, AUX), f32),
            pltpu.VMEM((outs, 2, chips * rows, nc), f32),
            pltpu.VMEM((outs, chips * rows, nc), f32),
            pltpu.VMEM((outs, chips, rows, nc), bf16),
            pltpu.VMEM((outs, chips, rows, nc), bf16),
            dma((units,)), dma((SLOTS,)), dma((SLOTS,)), dma((outs,)),
            dma((units,)), dma((units,)), dma((units,)), dma((units,)),
            dma((outs,)), dma((outs,)), dma((outs,)), dma((outs,)),
            dma((2,)), dma((2,)),
        ],
        compiler_params=pltpu.CompilerParams(
            collective_id=0, has_side_effects=True, vmem_limit_bytes=67_043_328
        ),
    )(tokens, routes, gates, wg, wu, wd)


def solution(mesh):
    placed = (
        P(("groups", "ep"), None),
        P(("groups", "ep"), None),
        P(("groups", "ep"), None),
        P(None, "ep"),
        P(None, "ep"),
        P("ep", None),
    )
    return jax.shard_map(
        layer, mesh=mesh, in_specs=placed, out_specs=P(("groups", "ep"), None), check_vma=False
    )
```

```python
import functools

import jax
import jax.numpy as jnp
from jax import lax
from jax.experimental import pallas as pl
from jax.experimental.pallas import tpu as pltpu
from jax.sharding import PartitionSpec as P

EXPERTS = 16
SLOTS = 3
AUX = 128


def piece(total, want):
    size = want
    while total % size:
        size //= 2
    return size


def kernel(
    devices, kc, nc, tile,
    tokens, routes, gates, wg, wu, wd, out,
    ring_g, ring_u, down, rx, ax, xf, xb, acc_g, acc_u, hid, share, mine, theirs, sbuf, rbuf,
    tok_sem, g_sem, u_sem, d_sem,
    tx_send, tx_recv, re_send, re_recv, ob_send, ob_recv, rt_send, rt_recv, ax_send, ax_recv,
):
    rows, width = tokens.shape
    hidden = wg.shape[1]
    chips = devices // 2
    units, outs = width // kc, width // nc
    me = lax.axis_index("ep")
    chip, core = me // 2, me % 2
    other = 1 - core
    peer = chip * 2 + other
    mates = chips * rows

    def remote(src, dst, send, recv, dev):
        return pltpu.make_async_remote_copy(
            src_ref=src, dst_ref=dst, send_sem=send, recv_sem=recv,
            device_id={"ep": dev}, device_id_type=pl.DeviceIdType.MESH,
        )

    def load_tokens(j):
        return pltpu.make_async_copy(
            tokens.at[:, pl.ds(j * kc, kc)], rx.at[j, core, chip], tok_sem.at[j]
        )

    def load_g(j):
        s = j % SLOTS
        return pltpu.make_async_copy(wg.at[pl.ds(j * kc, kc), :], ring_g.at[s], g_sem.at[s])

    def load_u(j):
        s = j % SLOTS
        return pltpu.make_async_copy(wu.at[pl.ds(j * kc, kc), :], ring_u.at[s], u_sem.at[s])

    def load_d(c):
        return pltpu.make_async_copy(wd.at[:, pl.ds(c * nc, nc)], down.at[c], d_sem.at[c])

    for j in range(units):
        load_tokens(j).start()
    for j in range(min(SLOTS, units)):
        load_g(j).start()
        load_u(j).start()
    issued = min(2, outs)
    for c in range(issued):
        load_d(c).start()

    barrier = pltpu.get_barrier_semaphore()
    pl.semaphore_signal(barrier, inc=1, device_id={"ep": peer}, device_id_type=pl.DeviceIdType.MESH)

    @pl.loop(1, chips)
    def _(i):
        to = lax.rem(chip + i, chips) * 2 + core
        pl.semaphore_signal(barrier, inc=1, device_id={"ep": to}, device_id_type=pl.DeviceIdType.MESH)

    lane = lax.broadcasted_iota(jnp.int32, (rows, AUX), 1)
    name = jnp.where(lane < EXPERTS, lane, lane - EXPERTS)
    weight = jnp.zeros((rows, AUX), jnp.float32)
    for k in range(routes.shape[1]):
        weight = weight + jnp.where(routes[:, k : k + 1] == name, gates[:, k : k + 1], 0.0)
    high = weight.astype(jnp.bfloat16).astype(jnp.float32)
    ax[core, chip] = jnp.where(
        lane < EXPERTS, high, jnp.where(lane < 2 * EXPERTS, weight - high, 0.0)
    ).astype(jnp.bfloat16)

    pl.semaphore_wait(barrier, chips)

    for j in range(units):
        load_tokens(j).wait()

        @pl.loop(1, chips)
        def _(i):
            to = lax.rem(chip + i, chips) * 2 + core
            remote(rx.at[j, core, chip], rx.at[j, core, chip], tx_send.at[j], tx_recv.at[j], to).start()

    @pl.loop(1, chips)
    def _(i):
        to = lax.rem(chip + i, chips) * 2 + core
        remote(ax.at[core, chip], ax.at[core, chip], ax_send.at[0], ax_recv.at[0], to).start()

    def many(ref, sem):
        return pltpu.make_async_copy(ref, ref, sem)

    def relay(j):
        return remote(rx.at[j, core], rx.at[j, core], re_send.at[j], re_recv.at[j], peer)

    relay_aux = remote(ax.at[core], ax.at[core], ax_send.at[1], ax_recv.at[1], peer)

    def forward(j):
        many(rx.at[j, 0, pl.ds(0, chips - 1)], tx_recv.at[j]).wait()
        relay(j).start()

    forward(0)
    for j in range(units):
        if j + 1 < units:
            forward(j + 1)
        else:
            many(ax.at[0, pl.ds(0, chips - 1)], ax_recv.at[0]).wait()
            relay_aux.start()
        relay(j).wait_recv()
        for half in range(2):
            @pl.loop(0, chips // 2)
            def _(b):
                pair = jnp.concatenate(
                    [rx[j, half, 2 * b].astype(jnp.float32), rx[j, half, 2 * b + 1].astype(jnp.float32)], axis=0
                )
                at = pl.multiple_of(half * mates + b * 2 * rows, 2 * rows)
                xf[pl.ds(at, 2 * rows), :] = pair
        xb[...] = xf[...].astype(jnp.bfloat16)
        load_g(j).wait()
        load_u(j).wait()
        s = j % SLOTS

        @pl.loop(0, hidden // tile, unroll=True)
        def _(n):
            cols = pl.ds(pl.multiple_of(n * tile, tile), tile)
            pg = jnp.dot(xb[...], ring_g[s, :, cols], preferred_element_type=jnp.float32)
            pu = jnp.dot(xb[...], ring_u[s, :, cols], preferred_element_type=jnp.float32)
            if j == 0:
                acc_g[:, cols] = pg
                acc_u[:, cols] = pu
            elif j < units - 1:
                acc_g[:, cols] += pg
                acc_u[:, cols] += pu
            else:
                g = acc_g[:, cols] + pg
                u = acc_u[:, cols] + pu
                hid[:, cols] = (g / (1.0 + jnp.exp(-g)) * u).astype(jnp.bfloat16)

        if j + SLOTS < units:
            load_g(j + SLOTS).start()
            load_u(j + SLOTS).start()
        goal = outs if j + SLOTS + 1 >= units else min(outs, issued + 1)
        while issued < goal:
            load_d(issued).start()
            issued += 1
    while issued < outs:
        load_d(issued).start()
        issued += 1

    relay_aux.wait_recv()
    expert = me // (devices // EXPERTS)
    spot = lax.broadcasted_iota(jnp.int32, (2 * rows, AUX), 1)
    hot = (spot == expert) | (spot == expert + EXPERTS)
    for half in range(2):
        @pl.loop(0, chips // 2)
        def _(b):
            pair = jnp.concatenate(
                [ax[half, 2 * b].astype(jnp.float32), ax[half, 2 * b + 1].astype(jnp.float32)], axis=0
            )
            at = pl.multiple_of(half * mates + b * 2 * rows, 2 * rows)
            total = jnp.sum(jnp.where(hot, pair, 0.0), axis=1, keepdims=True)
            share[pl.ds(at, 2 * rows), :] = jnp.broadcast_to(total, (2 * rows, AUX))

    def swap(c):
        return remote(mine.at[c, other], theirs.at[c], ob_send.at[c], ob_recv.at[c], peer)

    def give(c):
        swap(c).wait_recv()

        @pl.loop(0, chips // 2)
        def _(b):
            at = pl.multiple_of(b * 2 * rows, 2 * rows)
            both = mine[c, core, pl.ds(at, 2 * rows), :] + theirs[c, pl.ds(at, 2 * rows), :]
            sbuf[c, 2 * b] = both[:rows].astype(jnp.bfloat16)
            sbuf[c, 2 * b + 1] = both[rows:].astype(jnp.bfloat16)

        @pl.loop(1, chips)
        def _(i):
            dest = lax.rem(chip + i, chips)
            remote(
                sbuf.at[c, dest], rbuf.at[c, chip], rt_send.at[c], rt_recv.at[c], dest * 2 + core
            ).start()

        rbuf[c, chip] = sbuf[c, chip]

    sub = min(tile, nc)
    for c in range(outs):
        load_d(c).wait()

        @pl.loop(0, nc // sub, unroll=True)
        def _(n):
            cols = pl.ds(pl.multiple_of(n * sub, sub), sub)
            o = jnp.dot(hid[...], down[c, :, cols], preferred_element_type=jnp.float32)
            o = o * share[:, :1]
            mine[c, 0, :, cols] = o[:mates]
            mine[c, 1, :, cols] = o[mates:]

        swap(c).start()
        if c > 0:
            give(c - 1)
    give(outs - 1)

    for c in range(outs):
        many(rbuf.at[c, pl.ds(0, chips - 1)], rt_recv.at[c]).wait()
        total = rbuf[c, 0].astype(jnp.float32)
        if chips <= 16:
            for b in range(1, chips):
                total = total + rbuf[c, b].astype(jnp.float32)
        else:
            total = lax.fori_loop(1, chips, lambda b, t: t + rbuf[c, b].astype(jnp.float32), total)
        out[:, c * nc : (c + 1) * nc] = total.astype(jnp.bfloat16)

    for j in range(units):
        many(rx.at[j, 0, pl.ds(0, chips - 1)], tx_send.at[j]).wait()
        relay(j).wait_send()
    many(ax.at[0, pl.ds(0, chips - 1)], ax_send.at[0]).wait()
    relay_aux.wait_send()
    for c in range(outs):
        swap(c).wait_send()
        many(rbuf.at[c, pl.ds(0, chips - 1)], rt_send.at[c]).wait()


def layer(tokens, routes, gates, wg, wu, wd):
    devices = lax.axis_size("ep")
    rows, width = tokens.shape
    hidden = wg.shape[1]
    chips = devices // 2
    kc, nc = piece(width, 1024), piece(width, 1024)
    tile = piece(hidden, 512)
    units, outs = width // kc, width // nc
    batch = devices * rows
    bf16, f32 = jnp.bfloat16, jnp.float32
    dma = pltpu.SemaphoreType.DMA
    anywhere = pl.BlockSpec(memory_space=pl.ANY)
    vmem = pl.BlockSpec(memory_space=pltpu.VMEM)
    return pl.pallas_call(
        functools.partial(kernel, devices, kc, nc, tile),
        out_shape=jax.ShapeDtypeStruct((rows, width), bf16),
        in_specs=[anywhere, vmem, vmem, anywhere, anywhere, anywhere],
        out_specs=vmem,
        scratch_shapes=[
            pltpu.VMEM((SLOTS, kc, hidden), bf16),
            pltpu.VMEM((SLOTS, kc, hidden), bf16),
            pltpu.VMEM((outs, hidden, nc), bf16),
            pltpu.VMEM((units, 2, chips, rows, kc), bf16),
            pltpu.VMEM((2, chips, rows, AUX), bf16),
            pltpu.VMEM((batch, kc), f32),
            pltpu.VMEM((batch, kc), bf16),
            pltpu.VMEM((batch, hidden), f32),
            pltpu.VMEM((batch, hidden), f32),
            pltpu.VMEM((batch, hidden), bf16),
            pltpu.VMEM((batch, AUX), f32),
            pltpu.VMEM((outs, 2, chips * rows, nc), f32),
            pltpu.VMEM((outs, chips * rows, nc), f32),
            pltpu.VMEM((outs, chips, rows, nc), bf16),
            pltpu.VMEM((outs, chips, rows, nc), bf16),
            dma((units,)), dma((SLOTS,)), dma((SLOTS,)), dma((outs,)),
            dma((units,)), dma((units,)), dma((units,)), dma((units,)),
            dma((outs,)), dma((outs,)), dma((outs,)), dma((outs,)),
            dma((2,)), dma((2,)),
        ],
        compiler_params=pltpu.CompilerParams(
            collective_id=0, has_side_effects=True, vmem_limit_bytes=67_043_328
        ),
    )(tokens, routes, gates, wg, wu, wd)


def solution(mesh):
    placed = (
        P(("groups", "ep"), None),
        P(("groups", "ep"), None),
        P(("groups", "ep"), None),
        P(None, "ep"),
        P(None, "ep"),
        P("ep", None),
    )
    return jax.shard_map(
        layer, mesh=mesh, in_specs=placed, out_specs=P(("groups", "ep"), None), check_vma=False
    )
```
